8 devices in a mesh: rep: 1 (over z), pp: 8 (over x, y, core).
Axes of the slice: x: 2, y: 2, z: 1, core: 2. Of those that a mesh axis runs over, the one named last changes fastest.
Arguments:
- x: bfloat16 [16, 512, 640], P('rep')
- dy: bfloat16 [16, 512, 640], P('rep')
- w_gate: bfloat16 [8, 640, 1536], P('pp')
- w_up: bfloat16 [8, 640, 1536], P('pp')
- w_down: bfloat16 [8, 1536, 640], P('pp')
Outputs:
- output 1: bfloat16 [8, 640, 1536], P(('rep', 'pp'))
- output 2: bfloat16 [8, 640, 1536], P(('rep', 'pp'))
- output 3: bfloat16 [8, 1536, 640], P(('rep', 'pp'))
All inputs are finite; a program needn't handle non-finite values.
Results may differ from the reference program's by a relative error of at most 0.0288.
Values are sent between devices in bfloat16 or wider.
A program may use at most 2 GiB of HBM per device.

```python
import jax
import jax.numpy as jnp
from jax import lax

MICRO = 16
TOKENS = 512
D = 640
FF = 1536
LAYERS = 8
NAMES = ("w_gate", "w_up", "w_down")
SHAPES = {"w_gate": (LAYERS, D, FF), "w_up": (LAYERS, D, FF), "w_down": (LAYERS, FF, D)}


def bump(key, n, height):
    away = (jnp.arange(n, dtype=jnp.int32) - jax.random.randint(key, (), 0, n, jnp.int32)) % n
    return jnp.where(away < n // 8, height, 1.0)


def together(key, own, strength):
    shared = jax.random.normal(key, own.shape[1:], jnp.float32)
    return (own + strength * shared) * lax.rsqrt(1 + strength * strength)


def setup_inputs(seed: int = 0, part: int = 0) -> dict:
    kx, kdy, ka, kb, kz, kf, kh, kl, *kw = jax.random.split(jax.random.key(seed), 8 + len(NAMES))
    kx, kdy, ka, kb = (jax.random.fold_in(k, part) for k in (kx, kdy, ka, kb))
    shape = (MICRO, TOKENS, D)
    much_x, much_dy = jax.random.uniform(kz, (2,), jnp.float32, 0.0, 1.0)
    layers = 2.0 ** jax.random.uniform(kl, (LAYERS, 1, 1), jnp.float32, -1.0, 1.0)
    x = together(ka, jax.random.normal(kx, shape, jnp.float32), much_x) * bump(kf, D, 4.0)
    dy = together(kb, jax.random.normal(kdy, shape, jnp.float32), much_dy)
    drawn = {"x": x.astype(jnp.bfloat16), "dy": (dy * (MICRO * TOKENS) ** -0.5).astype(jnp.bfloat16)}
    for key, name in zip(kw, NAMES, strict=True):
        w = jax.random.normal(key, SHAPES[name], jnp.float32) * SHAPES[name][1] ** -0.5
        drawn[name] = (w * {"w_gate": 1.0, "w_up": bump(kh, FF, 4.0), "w_down": layers}[name]).astype(jnp.bfloat16)
    return drawn


def matmul(a, w):
    return jnp.dot(a, w, preferred_element_type=jnp.float32).astype(jnp.bfloat16)


def normed(h):
    wide = h.astype(jnp.float32)
    scale = lax.rsqrt(jnp.mean(wide**2, -1, keepdims=True) + 1e-6)
    return (wide * scale).astype(jnp.bfloat16)


def layer(h, w):
    a = normed(h)
    gate = jnp.dot(a, w["w_gate"], preferred_element_type=jnp.float32)
    up = jnp.dot(a, w["w_up"], preferred_element_type=jnp.float32)
    return h + matmul((jax.nn.silu(gate) * up).astype(jnp.bfloat16), w["w_down"])


def stack(weights, h):
    return lax.scan(lambda h, w: (layer(h, w), None), h, weights)[0]


def reference(x, dy, w_gate, w_up, w_down):
    weights = dict(zip(NAMES, (w_gate, w_up, w_down), strict=True))

    def take(so_far, one):
        h, by_y = one
        _, back = jax.vjp(lambda w: stack(w, h), weights)
        return jax.tree.map(lambda total, term: total + term.astype(jnp.float32), so_far, back(by_y)[0]), None

    none_yet = {name: jnp.zeros(w.shape, jnp.float32) for name, w in weights.items()}
    by_weights, _ = lax.scan(take, none_yet, (x, dy))
    return tuple(by_weights[name].astype(jnp.bfloat16) for name in NAMES)
```

```python
import functools

import jax
import jax.numpy as jnp
from jax import lax
from jax.experimental import pallas as pl
from jax.experimental.pallas import tpu as pltpu
from jax.sharding import PartitionSpec as P

BF, F32 = jnp.bfloat16, jnp.float32
MESH = pl.DeviceIdType.MESH
NN = (((1,), (0,)), ((), ()))
NT = (((1,), (1,)), ((), ()))
TN = (((0,), (0,)), ((), ()))
BLOCK = 256
WIDTH = 256
T = 256


def dot(a, b, dims=NN):
    return lax.dot_general(a, b, dims, preferred_element_type=F32)


def scale_of(wide):
    return lax.rsqrt(jnp.mean(wide * wide, 0, keepdims=True) + 1e-6)


def kernel(stages, x, dy, wg_in, wu_in, wd_in, wg_out, wu_out, wd_out, gu_hbm,
           wg, wu, wd, tg, tu, td, h, dh, gu, dg, du, pb, ab, pf, y_out, dh_out, fresh,
           w_sem, x_sem, gu_put, gu_get, y_send, y_recv, dh_send, dh_recv):
    me = lax.axis_index("pp")
    last = stages - 1
    micro, tokens, d = x.shape
    ff = wg.shape[1]
    per = tokens // T
    chunks = micro * per
    right, left = lax.rem(me + 1, stages), lax.rem(me + stages - 1, stages)
    ahead = per * (last - me)
    spill = ahead > 3

    def chunk_of(array, c):
        return array.at[c // per, pl.ds(pl.multiple_of(c % per * T, T), T), :]

    def load(array, c):
        return pltpu.make_async_copy(chunk_of(array, c), fresh.at[c % 2], x_sem.at[c % 2])

    def send_y(c):
        return pltpu.make_async_remote_copy(
            src_ref=y_out.at[c % 2], dst_ref=h.at[c], send_sem=y_send.at[c % 2], recv_sem=y_recv.at[c],
            device_id={"pp": right}, device_id_type=MESH)

    def send_dh(c):
        return pltpu.make_async_remote_copy(
            src_ref=dh_out.at[c % 2], dst_ref=dh.at[c], send_sem=dh_send.at[c % 2], recv_sem=dh_recv.at[c],
            device_id={"pp": left}, device_id_type=MESH)

    def put_gu(c):
        return pltpu.make_async_copy(gu.at[c % 2], gu_hbm.at[c], gu_put.at[c % 2])

    def get_gu(c):
        return pltpu.make_async_copy(gu_hbm.at[c], gu.at[2 + c % 2], gu_get.at[c % 2])

    barrier = pltpu.get_barrier_semaphore()

    @pl.when(me > 0)
    def _():
        pl.semaphore_signal(barrier, inc=1, device_id={"pp": left}, device_id_type=MESH)

    @pl.when(me < last)
    def _():
        pl.semaphore_signal(barrier, inc=1, device_id={"pp": right}, device_id_type=MESH)

    w_copies = [pltpu.make_async_copy(s, t, w_sem.at[i]) for i, (s, t) in enumerate(((wg_in, wg), (wu_in, wu), (wd_in, wd)))]
    @pl.when(me == 0)
    def _():
        load(x, 0).start()
        load(x, 1).start()

    for copy in w_copies:
        copy.start()

    def clear():
        for total in (tg, tu, td):
            total[...] = jnp.zeros_like(total)

    @pl.when(me == last)
    def _():
        load(dy, 0).start()
        load(dy, 1).start()

        def turn(c, _):
            load(dy, c).wait()
            dh[c] = fresh[c % 2].T

            @pl.when(c + 2 < chunks)
            def _():
                load(dy, c + 2).start()

            return 0

        lax.fori_loop(0, chunks, turn, 0)

    @pl.when(me > 0)
    def _():
        clear()

    for copy in w_copies:
        copy.wait()

    pl.semaphore_wait(barrier, jnp.where((me > 0) & (me < last), 2, 1))

    def up_and_gate(c, down):
        slot = jnp.where(spill, c % 2, c % 4)
        wide = h[c].astype(F32)
        a = (wide * scale_of(wide)).astype(BF)
        for j in range(ff // BLOCK):
            here = pl.ds(j * BLOCK, BLOCK)
            gate, up = dot(wg[:, here], a, TN), dot(wu[:, here], a, TN)
            gu[slot, here, :] = gate
            gu[slot, pl.ds(ff + j * BLOCK, BLOCK), :] = up
            if down:
                pf[here, :] = (gate * jax.nn.sigmoid(gate) * up).astype(BF)
        if down:
            y_out[c % 2] = h[c] + dot(wd[...], pf[...], TN).astype(BF)

    def forward(c):
        @pl.when(me == 0)
        def _():
            load(x, c).wait()
            h[c] = fresh[c % 2].T

            @pl.when(c + 2 < chunks)
            def _():
                load(x, c + 2).start()

        @pl.when(me > 0)
        def _():
            send_y(c).wait_recv()

        @pl.when(me < last)
        def _():
            @pl.when(c >= 2)
            def _():
                send_y(c - 2).wait_send()

            up_and_gate(c, True)
            send_y(c).start()

        @pl.when(me == last)
        def _():
            up_and_gate(c, False)

        @pl.when(spill)
        def _():
            put_gu(c).start()

    def hidden_back(c):
        slot = jnp.where(spill, 2 + c % 2, c % 4)
        half = c % per
        by_y = dh[c]
        for j in range(ff // BLOCK):
            here = pl.ds(j * BLOCK, BLOCK)
            by_p = dot(wd[here, :], by_y).astype(BF).astype(F32)
            gate, up = gu[slot, here, :], gu[slot, pl.ds(ff + j * BLOCK, BLOCK), :]
            sig = jax.nn.sigmoid(gate)
            silu = gate * sig
            pb[half, here, :] = (silu * up).astype(BF)
            du[half, here, :] = (silu * by_p).astype(BF)
            dg[half, here, :] = (up * by_p * (sig + silu * (1 - sig))).astype(BF)

    def state_back(c):
        half = c % per
        wide = h[c].astype(F32)
        scale = scale_of(wide)
        ab[half] = (wide * scale).astype(BF)
        by_a = (dot(wg[...], dg[half]).astype(BF) + dot(wu[...], du[half]).astype(BF)).astype(F32)
        along = jnp.sum(by_a * wide, 0, keepdims=True) * (scale * scale * scale) * (1.0 / d)
        dh_out[c % 2] = dh[c] + (by_a * scale - wide * along).astype(BF)

    def backward(c):
        @pl.when(me < last)
        def _():
            send_dh(c).wait_recv()

        @pl.when(me > 0)
        def _():
            @pl.when(c >= 2)
            def _():
                send_dh(c - 2).wait_send()

            hidden_back(c)
            state_back(c)
            send_dh(c).start()

        @pl.when(me == 0)
        def _():
            hidden_back(c)
            wide = h[c].astype(F32)
            ab[c % per] = (wide * scale_of(wide)).astype(BF)

    def weights_back(m):
        first = m * per
        for j in range(ff // WIDTH):
            here = pl.ds(j * WIDTH, WIDTH)
            for lhs, at, rhs, total in ((ab, 0, dg, tg), (ab, 0, du, tu), (dh, first, pb, td)):
                term = sum(dot(lhs[at + i], rhs[i, here, :], NT) for i in range(per))
                total[:, here] += term.astype(BF).astype(F32)

    def step(t, _):
        c = t - ahead

        @pl.when(spill & (t >= 2) & (t < chunks + 2))
        def _():
            put_gu(t - 2).wait()

        @pl.when(spill & (c + 1 >= 0) & (c + 1 < chunks))
        def _():
            get_gu(c + 1).start()

        @pl.when(t < chunks)
        def _():
            forward(t)

        @pl.when((me == 0) & (t == 2))
        def _():
            clear()

        @pl.when(c >= 0)
        def _():
            @pl.when(spill)
            def _():
                get_gu(c).wait()

            backward(c)

            @pl.when(c % per == per - 1)
            def _():
                weights_back(c // per)

        return 0

    lax.fori_loop(0, chunks + ahead, step, 0)

    wg[...] = tg[...].astype(BF)
    out_g = pltpu.make_async_copy(wg, wg_out, w_sem.at[0])
    out_g.start()
    wu[...] = tu[...].astype(BF)
    out_u = pltpu.make_async_copy(wu, wu_out, w_sem.at[1])
    out_u.start()
    wd[...] = td[...].astype(BF).T
    out_d = pltpu.make_async_copy(wd, wd_out, w_sem.at[2])
    out_d.start()
    for copy in (out_g, out_u, out_d):
        copy.wait()

    @pl.when(me < last)
    def _():
        for c in (chunks - 2, chunks - 1):
            send_y(c).wait_send()

    @pl.when(me > 0)
    def _():
        for c in (chunks - 2, chunks - 1):
            send_dh(c).wait_send()


def solution(mesh):
    stages = mesh.shape["pp"]

    def step(x, dy, wg, wu, wd):
        micro, tokens, d = x.shape
        ff = wg.shape[2]
        per = tokens // T
        chunks = micro * per
        vmem, dma = pltpu.VMEM, pltpu.SemaphoreType.DMA
        hbm = pl.BlockSpec(memory_space=pl.ANY)
        outs = pl.pallas_call(
            functools.partial(kernel, stages),
            out_shape=(
                jax.ShapeDtypeStruct((d, ff), BF),
                jax.ShapeDtypeStruct((d, ff), BF),
                jax.ShapeDtypeStruct((ff, d), BF),
                jax.ShapeDtypeStruct((chunks, 2 * ff, T), F32),
            ),
            in_specs=[hbm] * 5,
            out_specs=[hbm] * 4,
            scratch_shapes=[
                vmem((d, ff), BF), vmem((d, ff), BF), vmem((ff, d), BF),
                vmem((d, ff), F32), vmem((d, ff), F32), vmem((d, ff), F32),
                vmem((chunks, d, T), BF), vmem((chunks, d, T), BF),
                vmem((4, 2 * ff, T), F32),
                vmem((per, ff, T), BF), vmem((per, ff, T), BF), vmem((per, ff, T), BF),
                vmem((per, d, T), BF), vmem((ff, T), BF),
                vmem((2, d, T), BF), vmem((2, d, T), BF), vmem((2, T, d), BF),
                dma((3,)), dma((2,)), dma((2,)), dma((2,)), dma((2,)), dma((chunks,)), dma((2,)), dma((chunks,)),
            ],
            compiler_params=pltpu.CompilerParams(collective_id=0, has_side_effects=True, vmem_limit_bytes=67043328),
        )(x, dy, wg[0], wu[0], wd[0])
        return tuple(o[None] for o in outs[:3])

    return jax.shard_map(
        step,
        mesh=mesh,
        in_specs=(P("rep", None, None),) * 2 + (P("pp", None, None),) * 3,
        out_specs=(P(("rep", "pp"), None, None),) * 3,
        check_vma=False,
    )
```

```python
import functools

import jax
import jax.numpy as jnp
from jax import lax
from jax.experimental import pallas as pl
from jax.experimental.pallas import tpu as pltpu
from jax.sharding import PartitionSpec as P

BF, F32 = jnp.bfloat16, jnp.float32
MESH = pl.DeviceIdType.MESH
NN = (((1,), (0,)), ((), ()))
NT = (((1,), (1,)), ((), ()))
TN = (((0,), (0,)), ((), ()))
FORTH, BACK = 256, 512
WIDTH = 256
T = 256
RING = 2
DIGITS = 10
ORDER = (
    (153391689, 153391689, 203821641, 176507172, 476398235, 458307794, 461977250, 325662370, 441296090, 325662355, 441296090, 3),
    (153391689, 153391689, 321720969, 172339849, 304980635, 323597467, 309143251, 457815195, 309143250, 111771),
    (153391689, 170168905, 423958218, 455647827, 292099786, 458036875, 309143250, 457815195, 309143250, 111771),
    (153391689, 438866505, 325362889, 442807433, 438871115, 438940299, 457778899, 443131546, 443131546, 111834),
    (170168905, 155493978, 321492170, 174404249, 174892627, 170435227, 170435227, 306783378, 460175067, 112347),
    (289706569, 439161947, 189576273, 292074698, 291837521, 455648970, 170435210, 306783370, 460175067, 112347),
    (291837001, 292135626, 439161499, 290300555, 170202187, 289972874, 289739857, 460137553, 460175067, 112347),
    (289780817, 191960155, 171029588, 474290394, 292430475, 170440332, 289809034, 289741073, 289739857, 460175067, 898843),
)


LATER = (16, 16, 16, 16, 8, 8, 6, 8)


ON, BY_ON = 0, (8, 9, 10, 11, 12, 14, 16, 18, 20, 22, 23, 25, 28, 30, 31)
OFF, BY_OFF = 7, (0, 1, 2, 4, 5, 7, 8, 13, 15, 16, 31)


def among(c, chosen):
    return sum([jnp.where(c == k, 1, 0) for k in chosen], jnp.int32(0)) > 0


def place(c, chosen):
    return sum([jnp.where(c == k, i, 0) for i, k in enumerate(chosen)], jnp.int32(0))


def nth(r, chosen):
    return sum([jnp.where(r == i, k, 0) for i, k in enumerate(chosen)], jnp.int32(0))


def dot(a, b, dims=NN):
    return lax.dot_general(a, b, dims, preferred_element_type=F32)


def scale_of(wide):
    return lax.rsqrt(jnp.mean(wide * wide, 0, keepdims=True) + 1e-6)


def kernel(stages, x, dy, wg_in, wu_in, wd_in, wg_out, wu_out, wd_out, gu_hbm, post, kept,
           wg, wu, wd, tg, tu, td, h, dh, gu, terms, pf, y_out, dh_out, fresh,
           w_sem, x_sem, gu_put, gu_get, y_send, y_recv, dh_send, dh_recv, post_recv, post_send, keep, fetch):
    me = lax.axis_index("pp")
    last = stages - 1
    micro, tokens, d = x.shape
    ff = wg.shape[1]
    per = tokens // T
    chunks = micro * per
    right, left = lax.rem(me + 1, stages), lax.rem(me + stages - 1, stages)
    spill = me < last - 1
    pairs = [(i, i + 1) for i in range(last)] + [(0, 3), (0, 4), (3, 7), (4, 7)]

    later = sum(jnp.where(me == s, number, 0) for s, number in enumerate(LATER))

    def chunk_of(array, c):
        return array.at[c >> 1, pl.ds(pl.multiple_of((c & 1) * T, T), T), :]

    def load(array, c):
        return pltpu.make_async_copy(chunk_of(array, c), fresh.at[c & 1], x_sem.at[c & 1])

    def send_y(c):
        return pltpu.make_async_remote_copy(
            src_ref=y_out.at[c & 1], dst_ref=h.at[c], send_sem=y_send.at[c & 1], recv_sem=y_recv.at[c],
            device_id={"pp": right}, device_id_type=MESH)

    def send_dh(c):
        return pltpu.make_async_remote_copy(
            src_ref=dh_out.at[c & 1], dst_ref=dh.at[c], send_sem=dh_send.at[c & 1], recv_sem=dh_recv.at[c],
            device_id={"pp": left}, device_id_type=MESH)

    def post_to(source, c, r, target):
        return pltpu.make_async_remote_copy(
            src_ref=source.at[c & 1], dst_ref=post.at[r], send_sem=(y_send if target == 0 else dh_send).at[c & 1],
            recv_sem=post_recv.at[r], device_id={"pp": target}, device_id_type=MESH)

    def post_on(r):
        return pltpu.make_async_remote_copy(
            src_ref=post.at[r], dst_ref=h.at[nth(r, BY_ON)], send_sem=post_send.at[r], recv_sem=y_recv.at[nth(r, BY_ON)],
            device_id={"pp": 4}, device_id_type=MESH)

    def post_back(r):
        return pltpu.make_async_remote_copy(
            src_ref=post.at[r], dst_ref=dh.at[nth(r, BY_OFF)], send_sem=post_send.at[r], recv_sem=dh_recv.at[nth(r, BY_OFF)],
            device_id={"pp": 3}, device_id_type=MESH)

    def keep_terms(m):
        return pltpu.make_async_copy(terms.at[m & 1], kept.at[m], keep.at[m & 1])

    def fetch_terms(m):
        return pltpu.make_async_copy(kept.at[m], terms.at[m & 1], fetch.at[m & 1])

    def put_gu(c):
        return pltpu.make_async_copy(gu.at[c & 1], gu_hbm.at[c], gu_put.at[c & 1])

    def get_gu(c):
        return pltpu.make_async_copy(gu_hbm.at[c], gu.at[2 + (c & 1)], gu_get.at[c & 1])

    barrier = pltpu.get_barrier_semaphore()

    for one, two in pairs:
        for here, there in ((one, two), (two, one)):
            @pl.when(me == here)
            def _():
                pl.semaphore_signal(barrier, inc=1, device_id={"pp": there}, device_id_type=MESH)

    w_copies = [pltpu.make_async_copy(s, t, w_sem.at[i]) for i, (s, t) in enumerate(((wg_in, wg), (wu_in, wu), (wd_in, wd)))]
    @pl.when(me == 0)
    def _():
        load(x, 0).start()
        load(x, 1).start()

    for copy in w_copies:
        copy.start()

    def clear():
        for total in (tg, tu, td):
            total[...] = jnp.zeros_like(total)

    @pl.when(me == last)
    def _():
        load(dy, 0).start()
        load(dy, 1).start()

        def turn(c, _):
            load(dy, c).wait()
            dh[c] = fresh[c & 1].T

            @pl.when(c + 2 < chunks)
            def _():
                load(dy, c + 2).start()

            return 0

        lax.fori_loop(0, chunks, turn, 0)

    @pl.when(me > 0)
    def _():
        clear()

    for copy in w_copies:
        copy.wait()

    pl.semaphore_wait(barrier, sum(jnp.where((me == one) | (me == two), 1, 0) for one, two in pairs))

    def up_and_gate(c, down):
        slot = jnp.where(spill, c & 1, c & 3)
        wide = h[c].astype(F32)
        a = (wide * scale_of(wide)).astype(BF)
        for j in range(ff // FORTH):
            here = pl.ds(j * FORTH, FORTH)
            gate, up = dot(wg[:, here], a, TN), dot(wu[:, here], a, TN)
            gu[slot, here, :] = gate
            gu[slot, pl.ds(ff + j * FORTH, FORTH), :] = up
            if down:
                pf[here, :] = (gate * jax.nn.sigmoid(gate) * up).astype(BF)
        if down:
            y_out[c & 1] = h[c] + dot(wd[...], pf[...], TN).astype(BF)

    def forward(c, put):
        @pl.when(spill & (c >= 2) & (put == c - 2))
        def _():
            put_gu(c - 2).wait()

        @pl.when(me == 0)
        def _():
            load(x, c).wait()
            h[c] = fresh[c & 1].T

            @pl.when(c + 2 < chunks)
            def _():
                load(x, c + 2).start()

        @pl.when(me > 0)
        def _():
            send_y(c).wait_recv()

        @pl.when(me < last)
        def _():
            @pl.when(c >= 2)
            def _():
                send_y(c - 2).wait_send()

            up_and_gate(c, True)

        @pl.when((me < last) & ~((me == 3) & among(c, BY_ON)))
        def _():
            send_y(c).start()

        @pl.when((me == 3) & among(c, BY_ON))
        def _():
            post_to(y_out, c, place(c, BY_ON), 0).start()

        @pl.when(me == last)
        def _():
            up_and_gate(c, False)

        @pl.when(spill)
        def _():
            put_gu(c).start()

        @pl.when(spill & (c == 2))
        def _():
            get_gu(0).start()

    def hidden_back(c):
        slot = jnp.where(spill, 2 + (c & 1), c & 3)
        at, half = (c >> 1) & 1, c & 1
        by_y = dh[c]
        for j in range(ff // BACK):
            here = pl.ds(j * BACK, BACK)
            by_p = dot(wd[here, :], by_y).astype(BF).astype(F32)
            gate, up = gu[slot, here, :], gu[slot, pl.ds(ff + j * BACK, BACK), :]
            sig = jax.nn.sigmoid(gate)
            silu = gate * sig
            terms[at, 2, half, here, :] = (silu * up).astype(BF)
            terms[at, 1, half, here, :] = (silu * by_p).astype(BF)
            terms[at, 0, half, here, :] = (up * by_p * (sig + silu * (1 - sig))).astype(BF)

    def state_back(c):
        at, half = (c >> 1) & 1, c & 1
        wide = h[c].astype(F32)
        scale = scale_of(wide)
        by_a = (dot(wg[...], terms[at, 0, half]).astype(BF) + dot(wu[...], terms[at, 1, half]).astype(BF)).astype(F32)
        along = jnp.sum(by_a * wide, 0, keepdims=True) * (scale * scale * scale) * (1.0 / d)
        dh_out[c & 1] = dh[c] + (by_a * scale - wide * along).astype(BF)
        h[c] = (wide * scale).astype(BF)

    def backward(c, put):
        for k in (c, c + 1):
            @pl.when(spill & (put <= k) & (k < chunks))
            def _():
                put_gu(k).wait()

        @pl.when(((c & 1) == 0) & ((c >> 1) >= later + 2))
        def _():
            keep_terms((c >> 1) - 2).wait()

        @pl.when(spill & (c + 1 < chunks))
        def _():
            get_gu(c + 1).start()

        @pl.when(spill)
        def _():
            get_gu(c).wait()

        @pl.when(me < last)
        def _():
            send_dh(c).wait_recv()

        @pl.when(me > 0)
        def _():
            @pl.when(c >= 2)
            def _():
                send_dh(c - 2).wait_send()

            hidden_back(c)
            state_back(c)

        @pl.when((me > 0) & ~((me == 4) & among(c, BY_OFF)))
        def _():
            send_dh(c).start()

        @pl.when((me == 4) & among(c, BY_OFF))
        def _():
            post_to(dh_out, c, place(c, BY_OFF), 7).start()

        @pl.when(((c & 1) == 1) & ((c >> 1) >= later))
        def _():
            keep_terms(c >> 1).start()

        @pl.when((c == chunks - 1) & (later < micro))
        def _():
            keep_terms(micro - 2).wait()
            fetch_terms(later).start()

        @pl.when(me == 0)
        def _():
            hidden_back(c)
            wide = h[c].astype(F32)
            h[c] = (wide * scale_of(wide)).astype(BF)

    def weights_back(n):
        m, half = n >> 1, n & 1

        @pl.when((half == 0) & (m >= later))
        def _():
            @pl.when(m == later)
            def _():
                keep_terms(micro - 1).wait()
                fetch_terms(later + 1).start()

            fetch_terms(m).wait()

        for j in range(ff // 2 // WIDTH):
            here = pl.ds(pl.multiple_of(half * (ff // 2) + j * WIDTH, WIDTH), WIDTH)
            for lhs, i, total in ((h, 0, tg), (h, 1, tu), (dh, 2, td)):
                term = sum(dot(lhs[m * per + k], terms[m & 1, i, k, here, :], NT) for k in range(per))
                total[:, here] += term.astype(BF).astype(F32)

        @pl.when((half == 1) & (m >= later) & (m + 2 < micro))
        def _():
            fetch_terms(m + 2).start()

    def hand_on(r):
        pltpu.make_async_remote_copy(
            src_ref=y_out.at[0], dst_ref=post.at[r], send_sem=y_send.at[0], recv_sem=post_recv.at[r],
            device_id={"pp": right}, device_id_type=MESH).wait_recv()

        @pl.when(me == 0)
        def _():
            post_on(r).start()

        @pl.when(me == last)
        def _():
            post_back(r).start()

    def word(q, carry):
        code = sum(jnp.where((me == s) & (q == i), number, 0) for s, row in enumerate(ORDER) for i, number in enumerate(row) if number)

        def operation(_, carry):
            code, on, back, done, handed, put = carry
            kind = code & 7

            @pl.when(kind == 1)
            def _():
                forward(on, put)

            @pl.when((kind == 1) & (me == 0) & (on == 2))
            def _():
                clear()

            @pl.when(kind == 2)
            def _():
                backward(back, put)

            @pl.when(kind == 3)
            def _():
                weights_back(done)

            @pl.when(kind == 4)
            def _():
                hand_on(handed)

            put = jnp.where(kind == 1, jnp.maximum(put, on - 1), put)
            put = jnp.where(kind == 2, jnp.maximum(put, jnp.minimum(back + 2, chunks)), put)
            one = [jnp.where(kind == k, 1, 0) for k in (1, 2, 3, 4)]
            return code >> 3, on + one[0], back + one[1], done + one[2], handed + one[3], put

        return lax.fori_loop(0, DIGITS, operation, (code, *carry))[1:]

    lax.fori_loop(0, max(len(row) for row in ORDER), word, (jnp.int32(0),) * 5)

    wg[...] = tg[...].astype(BF)
    out_g = pltpu.make_async_copy(wg, wg_out, w_sem.at[0])
    out_g.start()
    wu[...] = tu[...].astype(BF)
    out_u = pltpu.make_async_copy(wu, wu_out, w_sem.at[1])
    out_u.start()
    wd[...] = td[...].astype(BF).T
    out_d = pltpu.make_async_copy(wd, wd_out, w_sem.at[2])
    out_d.start()
    for copy in (out_g, out_u, out_d):
        copy.wait()

    @pl.when(me < last)
    def _():
        for c in (chunks - 2, chunks - 1):
            send_y(c).wait_send()

    @pl.when(me > 0)
    def _():
        for c in (chunks - 2, chunks - 1):
            send_dh(c).wait_send()

    def sent(r, _):
        post_on(r).wait_send()
        return 0

    lax.fori_loop(0, jnp.where(me == 0, len(BY_ON), jnp.where(me == last, len(BY_OFF), 0)), sent, 0)


def solution(mesh):
    stages = mesh.shape["pp"]

    def step(x, dy, wg, wu, wd):
        micro, tokens, d = x.shape
        ff = wg.shape[2]
        per = tokens // T
        chunks = micro * per
        vmem, dma = pltpu.VMEM, pltpu.SemaphoreType.DMA
        hbm = pl.BlockSpec(memory_space=pl.ANY)
        outs = pl.pallas_call(
            functools.partial(kernel, stages),
            out_shape=(
                jax.ShapeDtypeStruct((d, ff), BF),
                jax.ShapeDtypeStruct((d, ff), BF),
                jax.ShapeDtypeStruct((ff, d), BF),
                jax.ShapeDtypeStruct((chunks, 2 * ff, T), F32),
                jax.ShapeDtypeStruct((16, d, T), BF),
                jax.ShapeDtypeStruct((micro, 3, per, ff, T), BF),
            ),
            in_specs=[hbm] * 5,
            out_specs=[hbm] * 6,
            scratch_shapes=[
                vmem((d, ff), BF), vmem((d, ff), BF), vmem((ff, d), BF),
                vmem((d, ff), F32), vmem((d, ff), F32), vmem((d, ff), F32),
                vmem((chunks, d, T), BF), vmem((chunks, d, T), BF),
                vmem((4, 2 * ff, T), F32),
                vmem((RING, 3, per, ff, T), BF), vmem((ff, T), BF),
                vmem((2, d, T), BF), vmem((2, d, T), BF), vmem((2, T, d), BF),
                dma((3,)), dma((2,)), dma((2,)), dma((2,)), dma((2,)), dma((chunks,)), dma((2,)), dma((chunks,)), dma((16,)), dma((16,)), dma((2,)), dma((2,)),
            ],
            compiler_params=pltpu.CompilerParams(collective_id=0, has_side_effects=True, vmem_limit_bytes=67043328),
        )(x, dy, wg[0], wu[0], wd[0])
        return tuple(o[None] for o in outs[:3])

    return jax.shard_map(
        step,
        mesh=mesh,
        in_specs=(P("rep", None, None),) * 2 + (P("pp", None, None),) * 3,
        out_specs=(P(("rep", "pp"), None, None),) * 3,
        check_vma=False,
    )
```

```python
import functools

import jax
import jax.numpy as jnp
from jax import lax
from jax.experimental import pallas as pl
from jax.experimental.pallas import tpu as pltpu
from jax.sharding import PartitionSpec as P

BF, F32 = jnp.bfloat16, jnp.float32
MESH = pl.DeviceIdType.MESH
NN = (((1,), (0,)), ((), ()))
NT = (((1,), (1,)), ((), ()))
TN = (((0,), (0,)), ((), ()))
FORTH, BACK = 256, 512
WIDTH = 256
T = 256
RING = 2
DIGITS = 10
ORDER = (
    (153391689, 153391689, 203821641, 176507172, 476398235, 458307794, 461977250, 325662370, 441296090, 325662355, 441296090, 3),
    (153391689, 153391689, 321720969, 172339849, 304980635, 323597467, 309143251, 457815195, 309143250, 111771),
    (153391689, 170168905, 423958218, 455647827, 292099786, 458036875, 309143250, 457815195, 309143250, 111771),
    (153391689, 438866505, 325362889, 442807433, 438871115, 438940299, 457778899, 443131546, 443131546, 111834),
    (170168905, 155493978, 321492170, 174404249, 174892627, 170435227, 170435227, 306783378, 460175067, 112347),
    (289706569, 439161947, 189576273, 292074698, 291837521, 455648970, 170435210, 306783370, 460175067, 112347),
    (291837001, 292135626, 439161499, 290300555, 170202187, 289972874, 289739857, 460137553, 460175067, 112347),
    (289780817, 191960155, 171029588, 474290394, 292430475, 170440332, 289809034, 289741073, 289739857, 460175067, 898843),
)


LATER = (16, 16, 16, 16, 8, 8, 6, 8)


ON, BY_ON = 0, (8, 9, 10, 11, 12, 14, 16, 18, 20, 22, 23, 25, 28, 30, 31)
OFF, BY_OFF = 7, (0, 1, 2, 4, 5, 7, 8, 13, 15, 16, 31)


def among(c, chosen):
    return sum([jnp.where(c == k, 1, 0) for k in chosen], jnp.int32(0)) > 0


def place(c, chosen):
    return sum([jnp.where(c == k, i, 0) for i, k in enumerate(chosen)], jnp.int32(0))


def nth(r, chosen):
    return sum([jnp.where(r == i, k, 0) for i, k in enumerate(chosen)], jnp.int32(0))


def dot(a, b, dims=NN):
    return lax.dot_general(a, b, dims, preferred_element_type=F32)


def scale_of(wide):
    return lax.rsqrt(jnp.mean(wide * wide, 0, keepdims=True) + 1e-6)


def kernel(stages, x, dy, wg_in, wu_in, wd_in, wg_out, wu_out, wd_out, gu_hbm, post, kept,
           wg, wu, wd, tg, tu, td, h, dh, gu, terms, pf, y_out, dh_out, fresh,
           w_sem, x_sem, gu_put, gu_get, y_send, y_recv, dh_send, dh_recv, post_recv, post_send, keep, fetch):
    me = lax.axis_index("pp")
    last = stages - 1
    micro, tokens, d = x.shape
    ff = wg.shape[1]
    per = tokens // T
    chunks = micro * per
    right, left = lax.rem(me + 1, stages), lax.rem(me + stages - 1, stages)
    spill = me < last - 1
    pairs = [(i, i + 1) for i in range(last)] + [(0, 3), (0, 4), (3, 7), (4, 7)]

    later = sum(jnp.where(me == s, number, 0) for s, number in enumerate(LATER))

    def chunk_of(array, c):
        return array.at[c >> 1, pl.ds(pl.multiple_of((c & 1) * T, T), T), :]

    def load(array, c):
        return pltpu.make_async_copy(chunk_of(array, c), fresh.at[c & 1], x_sem.at[c & 1])

    def send_y(c):
        return pltpu.make_async_remote_copy(
            src_ref=y_out.at[c & 1], dst_ref=h.at[c], send_sem=y_send.at[c & 1], recv_sem=y_recv.at[c],
            device_id={"pp": right}, device_id_type=MESH)

    def send_dh(c):
        return pltpu.make_async_remote_copy(
            src_ref=dh_out.at[c & 1], dst_ref=dh.at[c], send_sem=dh_send.at[c & 1], recv_sem=dh_recv.at[c],
            device_id={"pp": left}, device_id_type=MESH)

    def post_to(source, c, r, target):
        return pltpu.make_async_remote_copy(
            src_ref=source.at[c & 1], dst_ref=post.at[r], send_sem=(y_send if target == 0 else dh_send).at[c & 1],
            recv_sem=post_recv.at[r], device_id={"pp": target}, device_id_type=MESH)

    def post_on(r):
        return pltpu.make_async_remote_copy(
            src_ref=post.at[r], dst_ref=h.at[nth(r, BY_ON)], send_sem=post_send.at[r], recv_sem=y_recv.at[nth(r, BY_ON)],
            device_id={"pp": 4}, device_id_type=MESH)

    def post_back(r):
        return pltpu.make_async_remote_copy(
            src_ref=post.at[r], dst_ref=dh.at[nth(r, BY_OFF)], send_sem=post_send.at[r], recv_sem=dh_recv.at[nth(r, BY_OFF)],
            device_id={"pp": 3}, device_id_type=MESH)

    def keep_terms(m):
        return pltpu.make_async_copy(terms.at[m & 1], kept.at[m], keep.at[m & 1])

    def fetch_terms(m):
        return pltpu.make_async_copy(kept.at[m], terms.at[m & 1], fetch.at[m & 1])

    def put_gu(c):
        return pltpu.make_async_copy(gu.at[c & 1], gu_hbm.at[c], gu_put.at[c & 1])

    def get_gu(c):
        return pltpu.make_async_copy(gu_hbm.at[c], gu.at[2 + (c & 1)], gu_get.at[c & 1])

    barrier = pltpu.get_barrier_semaphore()

    for one, two in pairs:
        for here, there in ((one, two), (two, one)):
            @pl.when(me == here)
            def _():
                pl.semaphore_signal(barrier, inc=1, device_id={"pp": there}, device_id_type=MESH)

    w_copies = [pltpu.make_async_copy(s, t, w_sem.at[i]) for i, (s, t) in enumerate(((wg_in, wg), (wu_in, wu), (wd_in, wd)))]
    @pl.when(me == 0)
    def _():
        load(x, 0).start()
        load(x, 1).start()

    for copy in w_copies:
        copy.start()

    def clear():
        for total in (tg, tu, td):
            total[...] = jnp.zeros_like(total)

    @pl.when(me == last)
    def _():
        load(dy, 0).start()
        load(dy, 1).start()

        def turn(c, _):
            load(dy, c).wait()
            dh[c] = fresh[c & 1].T

            @pl.when(c + 2 < chunks)
            def _():
                load(dy, c + 2).start()

            return 0

        lax.fori_loop(0, chunks, turn, 0)

    @pl.when(me > 0)
    def _():
        clear()

    for copy in w_copies:
        copy.wait()

    pl.semaphore_wait(barrier, sum(jnp.where((me == one) | (me == two), 1, 0) for one, two in pairs))

    def up_and_gate(c, down):
        slot = jnp.where(spill, c & 1, c & 3)
        wide = h[c].astype(F32)
        a = (wide * scale_of(wide)).astype(BF)
        for j in range(ff // FORTH):
            here = pl.ds(j * FORTH, FORTH)
            gate, up = dot(wg[:, here], a, TN), dot(wu[:, here], a, TN)
            gu[slot, here, :] = gate
            gu[slot, pl.ds(ff + j * FORTH, FORTH), :] = up
            if down:
                pf[here, :] = (gate * jax.nn.sigmoid(gate) * up).astype(BF)
        if down:
            y_out[c & 1] = h[c] + dot(wd[...], pf[...], TN).astype(BF)

    def before_forward(c, put):
        @pl.when(spill & (c >= 2) & (put == c - 2))
        def _():
            put_gu(c - 2).wait()

        @pl.when(me == 0)
        def _():
            load(x, c).wait()
            h[c] = fresh[c & 1].T

            @pl.when(c + 2 < chunks)
            def _():
                load(x, c + 2).start()

        @pl.when(me > 0)
        def _():
            send_y(c).wait_recv()

        @pl.when((me < last) & (c >= 2))
        def _():
            send_y(c - 2).wait_send()

    def after_forward(c):
        @pl.when(spill)
        def _():
            put_gu(c).start()

            @pl.when(c == 2)
            def _():
                get_gu(0).start()

    def forward(c, put):
        before_forward(c, put)

        @pl.when(me < last)
        def _():
            up_and_gate(c, True)

            @pl.when(me != 3)
            def _():
                send_y(c).start()

            @pl.when(me == 3)
            def _():
                relayed = among(c, BY_ON)

                @pl.when(~relayed)
                def _():
                    send_y(c).start()

                @pl.when(relayed)
                def _():
                    post_to(y_out, c, place(c, BY_ON), 0).start()

        @pl.when(me == last)
        def _():
            up_and_gate(c, False)

        after_forward(c)

    def hidden_back(c):
        slot = jnp.where(spill, 2 + (c & 1), c & 3)
        at, half = (c >> 1) & 1, c & 1
        by_y = dh[c]
        for j in range(ff // BACK):
            here = pl.ds(j * BACK, BACK)
            by_p = dot(wd[here, :], by_y).astype(BF).astype(F32)
            gate, up = gu[slot, here, :], gu[slot, pl.ds(ff + j * BACK, BACK), :]
            sig = jax.nn.sigmoid(gate)
            silu = gate * sig
            terms[at, 2, half, here, :] = (silu * up).astype(BF)
            terms[at, 1, half, here, :] = (silu * by_p).astype(BF)
            terms[at, 0, half, here, :] = (up * by_p * (sig + silu * (1 - sig))).astype(BF)

    def state_back(c):
        at, half = (c >> 1) & 1, c & 1
        wide = h[c].astype(F32)
        scale = scale_of(wide)
        by_a = (dot(wg[...], terms[at, 0, half]).astype(BF) + dot(wu[...], terms[at, 1, half]).astype(BF)).astype(F32)
        along = jnp.sum(by_a * wide, 0, keepdims=True) * (scale * scale * scale) * (1.0 / d)
        dh_out[c & 1] = dh[c] + (by_a * scale - wide * along).astype(BF)
        h[c] = (wide * scale).astype(BF)

    def before_backward(c, put):
        @pl.when(((c & 1) == 0) & ((c >> 1) >= later + 2))
        def _():
            keep_terms((c >> 1) - 2).wait()

        @pl.when(spill)
        def _():
            for k in (c, c + 1):
                @pl.when((put <= k) & (k < chunks))
                def _():
                    put_gu(k).wait()

            @pl.when(c + 1 < chunks)
            def _():
                get_gu(c + 1).start()

            get_gu(c).wait()

        @pl.when(me < last)
        def _():
            send_dh(c).wait_recv()

        @pl.when((me > 0) & (c >= 2))
        def _():
            send_dh(c - 2).wait_send()

    def after_backward(c):
        @pl.when(((c & 1) == 1) & ((c >> 1) >= later))
        def _():
            keep_terms(c >> 1).start()

            @pl.when(c == chunks - 1)
            def _():
                keep_terms(micro - 2).wait()
                fetch_terms(later).start()

    def backward(c, put):
        before_backward(c, put)

        @pl.when(me > 0)
        def _():
            hidden_back(c)
            state_back(c)

            @pl.when(me != 4)
            def _():
                send_dh(c).start()

            @pl.when(me == 4)
            def _():
                relayed = among(c, BY_OFF)

                @pl.when(~relayed)
                def _():
                    send_dh(c).start()

                @pl.when(relayed)
                def _():
                    post_to(dh_out, c, place(c, BY_OFF), 7).start()

        @pl.when(me == 0)
        def _():
            hidden_back(c)
            wide = h[c].astype(F32)
            h[c] = (wide * scale_of(wide)).astype(BF)

        after_backward(c)

    def add_terms(m, half):
        for j in range(ff // 2 // WIDTH):
            here = pl.ds(j * WIDTH, WIDTH)
            rows = pl.ds(pl.multiple_of(half * (ff // 2) + j * WIDTH, WIDTH), WIDTH)
            for lhs, i, total in ((h, 0, tg), (h, 1, tu), (dh, 2, td)):
                term = sum(dot(lhs[m * per + k], terms[m & 1, i, k, rows, :], NT) for k in range(per))
                total[half, :, here] += term.astype(BF).astype(F32)

    def weights_back(n):
        m, half = n >> 1, n & 1

        @pl.when((half == 0) & (m >= later))
        def _():
            @pl.when(m == later)
            def _():
                keep_terms(micro - 1).wait()
                fetch_terms(later + 1).start()

            fetch_terms(m).wait()

        add_terms(m, half)

        @pl.when((half == 1) & (m >= later) & (m + 2 < micro))
        def _():
            fetch_terms(m + 2).start()

    def hand_on(r):
        pltpu.make_async_remote_copy(
            src_ref=y_out.at[0], dst_ref=post.at[r], send_sem=y_send.at[0], recv_sem=post_recv.at[r],
            device_id={"pp": right}, device_id_type=MESH).wait_recv()

        @pl.when(me == 0)
        def _():
            post_on(r).start()

        @pl.when(me == last)
        def _():
            post_back(r).start()

    def word(q, carry):
        code = sum(jnp.where((me == s) & (q == i), number, 0) for s, row in enumerate(ORDER) for i, number in enumerate(row) if number)

        def operation(_, carry):
            code, on, back, done, handed, put = carry
            kind = code & 7

            @pl.when(kind == 1)
            def _():
                forward(on, put)

            @pl.when((kind == 1) & (me == 0) & (on == 2))
            def _():
                clear()

            @pl.when(kind == 2)
            def _():
                backward(back, put)

            @pl.when(kind == 3)
            def _():
                weights_back(done)

            @pl.when(kind == 4)
            def _():
                hand_on(handed)

            put = jnp.where(kind == 1, jnp.maximum(put, on - 1), put)
            put = jnp.where(kind == 2, jnp.maximum(put, jnp.minimum(back + 2, chunks)), put)
            one = [jnp.where(kind == k, 1, 0) for k in (1, 2, 3, 4)]
            return code >> 3, on + one[0], back + one[1], done + one[2], handed + one[3], put

        return lax.fori_loop(0, DIGITS, operation, (code, *carry))[1:]

    lax.fori_loop(0, max(len(row) for row in ORDER), word, (jnp.int32(0),) * 5)

    cut = ff // 2
    for i in (0, 1):
        wg[:, i * cut:(i + 1) * cut] = tg[i].astype(BF)
    out_g = pltpu.make_async_copy(wg, wg_out, w_sem.at[0])
    out_g.start()
    for i in (0, 1):
        wu[:, i * cut:(i + 1) * cut] = tu[i].astype(BF)
    out_u = pltpu.make_async_copy(wu, wu_out, w_sem.at[1])
    out_u.start()
    for i in (0, 1):
        wd[i * cut:(i + 1) * cut, :] = td[i].astype(BF).T
    out_d = pltpu.make_async_copy(wd, wd_out, w_sem.at[2])
    out_d.start()
    for copy in (out_g, out_u, out_d):
        copy.wait()

    @pl.when(me < last)
    def _():
        for c in (chunks - 2, chunks - 1):
            send_y(c).wait_send()

    @pl.when(me > 0)
    def _():
        for c in (chunks - 2, chunks - 1):
            send_dh(c).wait_send()

    def sent(r, _):
        post_on(r).wait_send()
        return 0

    lax.fori_loop(0, jnp.where(me == 0, len(BY_ON), jnp.where(me == last, len(BY_OFF), 0)), sent, 0)


def solution(mesh):
    stages = mesh.shape["pp"]

    def step(x, dy, wg, wu, wd):
        micro, tokens, d = x.shape
        ff = wg.shape[2]
        per = tokens // T
        chunks = micro * per
        vmem, dma = pltpu.VMEM, pltpu.SemaphoreType.DMA
        hbm = pl.BlockSpec(memory_space=pl.ANY)
        outs = pl.pallas_call(
            functools.partial(kernel, stages),
            out_shape=(
                jax.ShapeDtypeStruct((d, ff), BF),
                jax.ShapeDtypeStruct((d, ff), BF),
                jax.ShapeDtypeStruct((ff, d), BF),
                jax.ShapeDtypeStruct((chunks, 2 * ff, T), F32),
                jax.ShapeDtypeStruct((16, d, T), BF),
                jax.ShapeDtypeStruct((micro, 3, per, ff, T), BF),
            ),
            in_specs=[hbm] * 5,
            out_specs=[hbm] * 6,
            scratch_shapes=[
                vmem((d, ff), BF), vmem((d, ff), BF), vmem((ff, d), BF),
                vmem((2, d, ff // 2), F32), vmem((2, d, ff // 2), F32), vmem((2, d, ff // 2), F32),
                vmem((chunks, d, T), BF), vmem((chunks, d, T), BF),
                vmem((4, 2 * ff, T), F32),
                vmem((RING, 3, per, ff, T), BF), vmem((ff, T), BF),
                vmem((2, d, T), BF), vmem((2, d, T), BF), vmem((2, T, d), BF),
                dma((3,)), dma((2,)), dma((2,)), dma((2,)), dma((2,)), dma((chunks,)), dma((2,)), dma((chunks,)), dma((16,)), dma((16,)), dma((2,)), dma((2,)),
            ],
            compiler_params=pltpu.CompilerParams(collective_id=0, has_side_effects=True, vmem_limit_bytes=67043328),
        )(x, dy, wg[0], wu[0], wd[0])
        return tuple(o[None] for o in outs[:3])

    return jax.shard_map(
        step,
        mesh=mesh,
        in_specs=(P("rep", None, None),) * 2 + (P("pp", None, None),) * 3,
        out_specs=(P(("rep", "pp"), None, None),) * 3,
        check_vma=False,
    )
```

```python
import functools

import jax
import jax.numpy as jnp
from jax import lax
from jax.experimental import pallas as pl
from jax.experimental.pallas import tpu as pltpu
from jax.sharding import PartitionSpec as P

BF, F32 = jnp.bfloat16, jnp.float32
MESH = pl.DeviceIdType.MESH
NN = (((1,), (0,)), ((), ()))
NT = (((1,), (1,)), ((), ()))
TN = (((0,), (0,)), ((), ()))
FORTH, BACK = 256, 512
WIDTH = 256
T = 256
RING = 2
DIGITS = 10
ORDER = (
    (153391689, 153391689, 203821641, 345118793, 457852628, 340899092, 441562267, 325662355, 441296090, 325662355, 441296090, 3),
    (153391689, 153391689, 438866505, 426058329, 309143250, 457815195, 309143250, 457815195, 309143250, 111771),
    (153391689, 170168905, 289773137, 321205841, 174891659, 443131091, 323826906, 323826899, 457778323, 112347),
    (153391689, 287871561, 438638155, 174891722, 423990481, 443130970, 323826906, 323826899, 441300115, 112338),
    (170168905, 155529818, 325396169, 172275281, 455648969, 170435210, 306783314, 460137618, 460175067, 112347),
    (289706569, 174367835, 189076555, 156021395, 422094426, 289739929, 306750545, 460137618, 460175067, 112347),
    (174920777, 289710810, 172298890, 172298890, 289739850, 289739857, 457774161, 460175067, 460175067, 112347),
    (438875217, 208192603, 292172433, 205853788, 289739874, 170435212, 170435210, 438870666, 462272227, 460175067, 14043),
)


LATER = (16, 16, 12, 16, 6, 6, 2, 4)


ON, BY_ON = 0, (8, 9, 11, 12, 14, 16, 17, 18, 19, 21, 24, 25, 27, 28, 31)
OFF, BY_OFF = 7, (0, 1, 2, 3, 5, 6, 9, 26, 28)


def among(c, chosen):
    return sum([jnp.where(c == k, 1, 0) for k in chosen], jnp.int32(0)) > 0


def place(c, chosen):
    return sum([jnp.where(c == k, i, 0) for i, k in enumerate(chosen)], jnp.int32(0))


def nth(r, chosen):
    return sum([jnp.where(r == i, k, 0) for i, k in enumerate(chosen)], jnp.int32(0))


def dot(a, b, dims=NN):
    return lax.dot_general(a, b, dims, preferred_element_type=F32)


def scale_of(wide):
    return lax.rsqrt(jnp.mean(wide * wide, 0, keepdims=True) + 1e-6)


def kernel(stages, x, dy, wg_in, wu_in, wd_in, wg_out, wu_out, wd_out, gu_hbm, post, kept,
           wg, wu, wd, tg, tu, td, h, dh, gu, terms, pf, y_out, dh_out, fresh,
           w_sem, x_sem, gu_put, gu_get, y_send, y_recv, dh_send, dh_recv, post_recv, post_send, keep, fetch):
    me = lax.axis_index("pp")
    last = stages - 1
    micro, tokens, d = x.shape
    ff = wg.shape[1]
    per = tokens // T
    chunks = micro * per
    right, left = lax.rem(me + 1, stages), lax.rem(me + stages - 1, stages)
    spill = me < last - 1
    pairs = [(i, i + 1) for i in range(last)] + [(0, 3), (0, 4), (3, 7), (4, 7)]

    later = sum(jnp.where(me == s, number, 0) for s, number in enumerate(LATER))

    def chunk_of(array, c):
        return array.at[c >> 1, pl.ds(pl.multiple_of((c & 1) * T, T), T), :]

    def load(array, c):
        return pltpu.make_async_copy(chunk_of(array, c), fresh.at[c & 1], x_sem.at[c & 1])

    def send_y(c):
        return pltpu.make_async_remote_copy(
            src_ref=y_out.at[c & 3], dst_ref=h.at[c], send_sem=y_send.at[c & 3], recv_sem=y_recv.at[c],
            device_id={"pp": right}, device_id_type=MESH)

    def send_dh(c):
        return pltpu.make_async_remote_copy(
            src_ref=dh_out.at[c & 3], dst_ref=dh.at[c], send_sem=dh_send.at[c & 3], recv_sem=dh_recv.at[c],
            device_id={"pp": left}, device_id_type=MESH)

    def post_to(source, c, r, target):
        return pltpu.make_async_remote_copy(
            src_ref=source.at[c & 3], dst_ref=post.at[r], send_sem=(y_send if target == 0 else dh_send).at[c & 3],
            recv_sem=post_recv.at[r], device_id={"pp": target}, device_id_type=MESH)

    def post_on(r):
        return pltpu.make_async_remote_copy(
            src_ref=post.at[r], dst_ref=h.at[nth(r, BY_ON)], send_sem=post_send.at[r], recv_sem=y_recv.at[nth(r, BY_ON)],
            device_id={"pp": 4}, device_id_type=MESH)

    def post_back(r):
        return pltpu.make_async_remote_copy(
            src_ref=post.at[r], dst_ref=dh.at[nth(r, BY_OFF)], send_sem=post_send.at[r], recv_sem=dh_recv.at[nth(r, BY_OFF)],
            device_id={"pp": 3}, device_id_type=MESH)

    def keep_terms(m):
        return pltpu.make_async_copy(terms.at[m & 1], kept.at[m], keep.at[m & 1])

    def fetch_terms(m):
        return pltpu.make_async_copy(kept.at[m], terms.at[m & 1], fetch.at[m & 1])

    def put_gu(c):
        return pltpu.make_async_copy(gu.at[c & 1], gu_hbm.at[c], gu_put.at[c & 1])

    def get_gu(c):
        return pltpu.make_async_copy(gu_hbm.at[c], gu.at[2 + (c & 1)], gu_get.at[c & 1])

    barrier = pltpu.get_barrier_semaphore()

    for one, two in pairs:
        for here, there in ((one, two), (two, one)):
            @pl.when(me == here)
            def _():
                pl.semaphore_signal(barrier, inc=1, device_id={"pp": there}, device_id_type=MESH)

    w_copies = [pltpu.make_async_copy(s, t, w_sem.at[i]) for i, (s, t) in enumerate(((wg_in, wg), (wu_in, wu), (wd_in, wd)))]
    @pl.when(me == 0)
    def _():
        load(x, 0).start()
        load(x, 1).start()

    for copy in w_copies:
        copy.start()

    def clear():
        for total in (tg, tu, td):
            total[...] = jnp.zeros_like(total)

    @pl.when(me == last)
    def _():
        load(dy, 0).start()
        load(dy, 1).start()

        def turn(c, _):
            load(dy, c).wait()
            dh[c] = fresh[c & 1].T

            @pl.when(c + 2 < chunks)
            def _():
                load(dy, c + 2).start()

            return 0

        lax.fori_loop(0, chunks, turn, 0)

    @pl.when(me > 0)
    def _():
        clear()

    for copy in w_copies:
        copy.wait()

    pl.semaphore_wait(barrier, sum(jnp.where((me == one) | (me == two), 1, 0) for one, two in pairs))

    def up_and_gate(c, down):
        slot = jnp.where(spill, c & 1, c & 3)
        wide = h[c].astype(F32)
        a = (wide * scale_of(wide)).astype(BF)
        for j in range(ff // FORTH):
            here = pl.ds(j * FORTH, FORTH)
            gate, up = dot(wg[:, here], a, TN), dot(wu[:, here], a, TN)
            gu[slot, here, :] = gate
            gu[slot, pl.ds(ff + j * FORTH, FORTH), :] = up
            if down:
                pf[here, :] = (gate * jax.nn.sigmoid(gate) * up).astype(BF)
        if down:
            y_out[c & 3] = h[c] + dot(wd[...], pf[...], TN).astype(BF)

    def before_forward(c, put):
        @pl.when(spill & (c >= 2) & (put == c - 2))
        def _():
            put_gu(c - 2).wait()

        @pl.when(me == 0)
        def _():
            load(x, c).wait()
            h[c] = fresh[c & 1].T

            @pl.when(c + 2 < chunks)
            def _():
                load(x, c + 2).start()

        @pl.when(me > 0)
        def _():
            send_y(c).wait_recv()

        @pl.when((me < last) & (c >= 4))
        def _():
            send_y(c - 4).wait_send()

    def after_forward(c):
        @pl.when(spill)
        def _():
            put_gu(c).start()

            @pl.when(c == 2)
            def _():
                get_gu(0).start()

    def forward(c, put):
        before_forward(c, put)

        @pl.when(me < last)
        def _():
            up_and_gate(c, True)

            @pl.when(me != 3)
            def _():
                send_y(c).start()

            @pl.when(me == 3)
            def _():
                relayed = among(c, BY_ON)

                @pl.when(~relayed)
                def _():
                    send_y(c).start()

                @pl.when(relayed)
                def _():
                    post_to(y_out, c, place(c, BY_ON), 0).start()

        @pl.when(me == last)
        def _():
            up_and_gate(c, False)

        after_forward(c)

    def hidden_back(c):
        slot = jnp.where(spill, 2 + (c & 1), c & 3)
        at, half = (c >> 1) & 1, c & 1
        by_y = dh[c]
        for j in range(ff // BACK):
            here = pl.ds(j * BACK, BACK)
            by_p = dot(wd[here, :], by_y).astype(BF).astype(F32)
            gate, up = gu[slot, here, :], gu[slot, pl.ds(ff + j * BACK, BACK), :]
            sig = jax.nn.sigmoid(gate)
            silu = gate * sig
            terms[at, 2, half, here, :] = (silu * up).astype(BF)
            terms[at, 1, half, here, :] = (silu * by_p).astype(BF)
            terms[at, 0, half, here, :] = (up * by_p * (sig + silu * (1 - sig))).astype(BF)

    def state_back(c):
        at, half = (c >> 1) & 1, c & 1
        wide = h[c].astype(F32)
        scale = scale_of(wide)
        by_a = (dot(wg[...], terms[at, 0, half]).astype(BF) + dot(wu[...], terms[at, 1, half]).astype(BF)).astype(F32)
        along = jnp.sum(by_a * wide, 0, keepdims=True) * (scale * scale * scale) * (1.0 / d)
        dh_out[c & 3] = dh[c] + (by_a * scale - wide * along).astype(BF)
        h[c] = (wide * scale).astype(BF)

    def before_backward(c, put):
        @pl.when(((c & 1) == 0) & ((c >> 1) >= later + 2))
        def _():
            keep_terms((c >> 1) - 2).wait()

        @pl.when(spill)
        def _():
            for k in (c, c + 1):
                @pl.when((put <= k) & (k < chunks))
                def _():
                    put_gu(k).wait()

            @pl.when(c + 1 < chunks)
            def _():
                get_gu(c + 1).start()

            get_gu(c).wait()

        @pl.when(me < last)
        def _():
            send_dh(c).wait_recv()

        @pl.when((me > 0) & (c >= 4))
        def _():
            send_dh(c - 4).wait_send()

    def after_backward(c):
        @pl.when(((c & 1) == 1) & ((c >> 1) >= later))
        def _():
            keep_terms(c >> 1).start()

            @pl.when(c == chunks - 1)
            def _():
                keep_terms(micro - 2).wait()
                fetch_terms(later).start()

    def backward(c, put):
        before_backward(c, put)

        @pl.when(me > 0)
        def _():
            hidden_back(c)
            state_back(c)

            @pl.when(me != 4)
            def _():
                send_dh(c).start()

            @pl.when(me == 4)
            def _():
                relayed = among(c, BY_OFF)

                @pl.when(~relayed)
                def _():
                    send_dh(c).start()

                @pl.when(relayed)
                def _():
                    post_to(dh_out, c, place(c, BY_OFF), 7).start()

        @pl.when(me == 0)
        def _():
            hidden_back(c)
            wide = h[c].astype(F32)
            h[c] = (wide * scale_of(wide)).astype(BF)

        after_backward(c)

    def add_terms(m, half):
        for j in range(ff // 2 // WIDTH):
            here = pl.ds(j * WIDTH, WIDTH)
            rows = pl.ds(pl.multiple_of(half * (ff // 2) + j * WIDTH, WIDTH), WIDTH)
            for lhs, i, total in ((h, 0, tg), (h, 1, tu), (dh, 2, td)):
                term = sum(dot(lhs[m * per + k], terms[m & 1, i, k, rows, :], NT) for k in range(per))
                total[half, :, here] += term.astype(BF).astype(F32)

    def weights_back(n):
        m, half = n >> 1, n & 1

        @pl.when((half == 0) & (m >= later))
        def _():
            @pl.when(m == later)
            def _():
                keep_terms(micro - 1).wait()
                fetch_terms(later + 1).start()

            fetch_terms(m).wait()

        add_terms(m, half)

        @pl.when((half == 1) & (m >= later) & (m + 2 < micro))
        def _():
            fetch_terms(m + 2).start()

    def hand_on(r):
        pltpu.make_async_remote_copy(
            src_ref=y_out.at[0], dst_ref=post.at[r], send_sem=y_send.at[0], recv_sem=post_recv.at[r],
            device_id={"pp": right}, device_id_type=MESH).wait_recv()

        @pl.when(me == 0)
        def _():
            post_on(r).start()

        @pl.when(me == last)
        def _():
            post_back(r).start()

    def word(q, carry):
        code = sum(jnp.where((me == s) & (q == i), number, 0) for s, row in enumerate(ORDER) for i, number in enumerate(row) if number)

        def operation(_, carry):
            code, on, back, done, handed, put = carry
            kind = code & 7

            @pl.when(kind == 1)
            def _():
                forward(on, put)

            @pl.when((kind == 1) & (me == 0) & (on == 2))
            def _():
                clear()

            @pl.when(kind == 2)
            def _():
                backward(back, put)

            @pl.when(kind == 3)
            def _():
                weights_back(done)

            @pl.when(kind == 4)
            def _():
                hand_on(handed)

            put = jnp.where(kind == 1, jnp.maximum(put, on - 1), put)
            put = jnp.where(kind == 2, jnp.maximum(put, jnp.minimum(back + 2, chunks)), put)
            one = [jnp.where(kind == k, 1, 0) for k in (1, 2, 3, 4)]
            return code >> 3, on + one[0], back + one[1], done + one[2], handed + one[3], put

        return lax.fori_loop(0, DIGITS, operation, (code, *carry))[1:]

    lax.fori_loop(0, max(len(row) for row in ORDER), word, (jnp.int32(0),) * 5)

    cut = ff // 2
    for i in (0, 1):
        wg[:, i * cut:(i + 1) * cut] = tg[i].astype(BF)
    out_g = pltpu.make_async_copy(wg, wg_out, w_sem.at[0])
    out_g.start()
    for i in (0, 1):
        wu[:, i * cut:(i + 1) * cut] = tu[i].astype(BF)
    out_u = pltpu.make_async_copy(wu, wu_out, w_sem.at[1])
    out_u.start()
    for i in (0, 1):
        wd[i * cut:(i + 1) * cut, :] = td[i].astype(BF).T
    out_d = pltpu.make_async_copy(wd, wd_out, w_sem.at[2])
    out_d.start()
    for copy in (out_g, out_u, out_d):
        copy.wait()

    @pl.when(me < last)
    def _():
        for c in range(chunks - 4, chunks):
            send_y(c).wait_send()

    @pl.when(me > 0)
    def _():
        for c in range(chunks - 4, chunks):
            send_dh(c).wait_send()

    def sent(r, _):
        post_on(r).wait_send()
        return 0

    lax.fori_loop(0, jnp.where(me == 0, len(BY_ON), jnp.where(me == last, len(BY_OFF), 0)), sent, 0)


def hand_out(*refs):
    for source, target in zip(refs[:3], refs[3:]):
        target[0] = source[...]


def solution(mesh):
    stages = mesh.shape["pp"]

    def step(x, dy, wg, wu, wd):
        micro, tokens, d = x.shape
        ff = wg.shape[2]
        per = tokens // T
        chunks = micro * per
        vmem, dma = pltpu.VMEM, pltpu.SemaphoreType.DMA
        hbm = pl.BlockSpec(memory_space=pl.ANY)
        outs = pl.pallas_call(
            functools.partial(kernel, stages),
            out_shape=(
                jax.ShapeDtypeStruct((d, ff), BF),
                jax.ShapeDtypeStruct((d, ff), BF),
                jax.ShapeDtypeStruct((ff, d), BF),
                jax.ShapeDtypeStruct((chunks, 2 * ff, T), F32),
                jax.ShapeDtypeStruct((16, d, T), BF),
                jax.ShapeDtypeStruct((micro, 3, per, ff, T), BF),
            ),
            in_specs=[hbm] * 5,
            out_specs=[hbm] * 6,
            scratch_shapes=[
                vmem((d, ff), BF), vmem((d, ff), BF), vmem((ff, d), BF),
                vmem((2, d, ff // 2), F32), vmem((2, d, ff // 2), F32), vmem((2, d, ff // 2), F32),
                vmem((chunks, d, T), BF), vmem((chunks, d, T), BF),
                vmem((4, 2 * ff, T), F32),
                vmem((RING, 3, per, ff, T), BF), vmem((ff, T), BF),
                vmem((4, d, T), BF), vmem((4, d, T), BF), vmem((2, T, d), BF),
                dma((3,)), dma((2,)), dma((2,)), dma((2,)), dma((4,)), dma((chunks,)), dma((4,)), dma((chunks,)), dma((16,)), dma((16,)), dma((2,)), dma((2,)),
            ],
            compiler_params=pltpu.CompilerParams(collective_id=0, has_side_effects=True, vmem_limit_bytes=67043328),
        )(x, dy, wg[0], wu[0], wd[0])
        cut = 2
        shapes = ((d, ff), (d, ff), (ff, d))
        return pl.pallas_call(
            hand_out,
            grid=(cut,),
            out_shape=tuple(jax.ShapeDtypeStruct((1, *shape), BF) for shape in shapes),
            in_specs=[pl.BlockSpec((r // cut, c), lambda i: (i, 0)) for r, c in shapes],
            out_specs=tuple(pl.BlockSpec((1, r // cut, c), lambda i: (0, i, 0)) for r, c in shapes),
        )(*outs[:3])

    return jax.shard_map(
        step,
        mesh=mesh,
        in_specs=(P("rep", None, None),) * 2 + (P("pp", None, None),) * 3,
        out_specs=(P(("rep", "pp"), None, None),) * 3,
        check_vma=False,
    )
```

```python
import functools

import jax
import jax.numpy as jnp
from jax import lax
from jax.experimental import pallas as pl
from jax.experimental.pallas import tpu as pltpu
from jax.sharding import PartitionSpec as P

BF, F32 = jnp.bfloat16, jnp.float32
MESH = pl.DeviceIdType.MESH
NN = (((1,), (0,)), ((), ()))
NT = (((1,), (1,)), ((), ()))
TN = (((0,), (0,)), ((), ()))
FORTH, BACK = 256, 256
WIDTH = 256
T = 256
RING = 2
DIGITS = 10
ORDER = (
    (153391689, 153391689, 203821641, 345118793, 457852628, 340899092, 441562267, 325662355, 441296090, 325662355, 441296090, 3),
    (153391689, 153391689, 438866505, 426058329, 309143250, 457815195, 309143250, 457815195, 309143250, 111771),
    (153391689, 170168905, 289773137, 321205841, 174891659, 443131091, 323826906, 323826899, 457778323, 112347),
    (153391689, 287871561, 438638155, 174891722, 423990481, 443130970, 323826906, 323826899, 441300115, 112338),
    (170168905, 155529818, 325396169, 172275281, 455648969, 170435210, 306783314, 460137618, 460175067, 112347),
    (289706569, 174367835, 189076555, 156021395, 422094426, 289739929, 306750545, 460137618, 460175067, 112347),
    (174920777, 289710810, 172298890, 172298890, 289739850, 289739857, 457774161, 460175067, 460175067, 112347),
    (438875217, 208192603, 292172433, 205853788, 289739874, 170435212, 170435210, 438870666, 462272227, 460175067, 14043),
)


LATER = (16, 16, 12, 16, 6, 6, 2, 4)


ON, BY_ON = 0, (8, 9, 11, 12, 14, 16, 17, 18, 19, 21, 24, 25, 27, 28, 31)
OFF, BY_OFF = 7, (0, 1, 2, 3, 5, 6, 9, 26, 28)


def among(c, chosen):
    return sum([jnp.where(c == k, 1, 0) for k in chosen], jnp.int32(0)) > 0


def place(c, chosen):
    return sum([jnp.where(c == k, i, 0) for i, k in enumerate(chosen)], jnp.int32(0))


def nth(r, chosen):
    return sum([jnp.where(r == i, k, 0) for i, k in enumerate(chosen)], jnp.int32(0))


def dot(a, b, dims=NN):
    return lax.dot_general(a, b, dims, preferred_element_type=F32)


def scale_of(wide):
    return lax.rsqrt(jnp.mean(wide * wide, 0, keepdims=True) + 1e-6)


def kernel(stages, x, dy, wg_in, wu_in, wd_in, wg_out, wu_out, wd_out, gu_hbm, post, kept,
           wg, wu, wd, tg, tu, td, h, dh, gu, terms, pf, y_out, dh_out, fresh,
           w_sem, x_sem, gu_put, gu_get, y_send, y_recv, dh_send, dh_recv, post_recv, post_send, keep, fetch):
    me = lax.axis_index("pp")
    last = stages - 1
    micro, tokens, d = x.shape
    ff = wg.shape[1]
    per = tokens // T
    chunks = micro * per
    right, left = lax.rem(me + 1, stages), lax.rem(me + stages - 1, stages)
    spill = me < last - 1
    pairs = [(i, i + 1) for i in range(last)] + [(0, 3), (0, 4), (3, 7), (4, 7)]

    later = sum(jnp.where(me == s, number, 0) for s, number in enumerate(LATER))

    def chunk_of(array, c):
        return array.at[c >> 1, pl.ds(pl.multiple_of((c & 1) * T, T), T), :]

    def load(array, c):
        return pltpu.make_async_copy(chunk_of(array, c), fresh.at[c & 1], x_sem.at[c & 1])

    def send_y(c):
        return pltpu.make_async_remote_copy(
            src_ref=y_out.at[c & 3], dst_ref=h.at[c], send_sem=y_send.at[c & 3], recv_sem=y_recv.at[c],
            device_id={"pp": right}, device_id_type=MESH)

    def send_dh(c):
        return pltpu.make_async_remote_copy(
            src_ref=dh_out.at[c & 3], dst_ref=dh.at[c], send_sem=dh_send.at[c & 3], recv_sem=dh_recv.at[c],
            device_id={"pp": left}, device_id_type=MESH)

    def post_to(source, c, r, target):
        return pltpu.make_async_remote_copy(
            src_ref=source.at[c & 3], dst_ref=post.at[r], send_sem=(y_send if target == 0 else dh_send).at[c & 3],
            recv_sem=post_recv.at[r], device_id={"pp": target}, device_id_type=MESH)

    def post_on(r):
        return pltpu.make_async_remote_copy(
            src_ref=post.at[r], dst_ref=h.at[nth(r, BY_ON)], send_sem=post_send.at[r], recv_sem=y_recv.at[nth(r, BY_ON)],
            device_id={"pp": 4}, device_id_type=MESH)

    def post_back(r):
        return pltpu.make_async_remote_copy(
            src_ref=post.at[r], dst_ref=dh.at[nth(r, BY_OFF)], send_sem=post_send.at[r], recv_sem=dh_recv.at[nth(r, BY_OFF)],
            device_id={"pp": 3}, device_id_type=MESH)

    def keep_terms(m):
        return pltpu.make_async_copy(terms.at[m & 1], kept.at[m], keep.at[m & 1])

    def fetch_terms(m):
        return pltpu.make_async_copy(kept.at[m], terms.at[m & 1], fetch.at[m & 1])

    def put_gu(c):
        return pltpu.make_async_copy(gu.at[c & 1], gu_hbm.at[c], gu_put.at[c & 1])

    def get_gu(c):
        return pltpu.make_async_copy(gu_hbm.at[c], gu.at[2 + (c & 1)], gu_get.at[c & 1])

    barrier = pltpu.get_barrier_semaphore()

    for one, two in pairs:
        for here, there in ((one, two), (two, one)):
            @pl.when(me == here)
            def _():
                pl.semaphore_signal(barrier, inc=1, device_id={"pp": there}, device_id_type=MESH)

    w_copies = [pltpu.make_async_copy(s, t, w_sem.at[i]) for i, (s, t) in enumerate(((wg_in, wg), (wu_in, wu), (wd_in, wd)))]
    @pl.when(me == 0)
    def _():
        load(x, 0).start()
        load(x, 1).start()

    for copy in w_copies:
        copy.start()

    def clear():
        for total in (tg, tu, td):
            total[...] = jnp.zeros_like(total)

    @pl.when(me == last)
    def _():
        load(dy, 0).start()
        load(dy, 1).start()

        def turn(c, _):
            load(dy, c).wait()
            dh[c] = fresh[c & 1].T

            @pl.when(c + 2 < chunks)
            def _():
                load(dy, c + 2).start()

            return 0

        lax.fori_loop(0, chunks, turn, 0)

    @pl.when(me > 0)
    def _():
        clear()

    for copy in w_copies:
        copy.wait()

    pl.semaphore_wait(barrier, sum(jnp.where((me == one) | (me == two), 1, 0) for one, two in pairs))

    def up_and_gate(c, down):
        slot = jnp.where(spill, c & 1, c & 3)
        wide = h[c].astype(F32)
        a = (wide * scale_of(wide)).astype(BF)
        for j in range(ff // FORTH):
            here = pl.ds(j * FORTH, FORTH)
            gate, up = dot(wg[:, here], a, TN), dot(wu[:, here], a, TN)
            gu[slot, here, :] = gate
            gu[slot, pl.ds(ff + j * FORTH, FORTH), :] = up
            if down:
                pf[here, :] = (gate * jax.nn.sigmoid(gate) * up).astype(BF)
        if down:
            y_out[c & 3] = h[c] + dot(wd[...], pf[...], TN).astype(BF)

    def before_forward(c, put):
        @pl.when(spill & (c >= 2) & (put == c - 2))
        def _():
            put_gu(c - 2).wait()

        @pl.when(me == 0)
        def _():
            load(x, c).wait()
            h[c] = fresh[c & 1].T

            @pl.when(c + 2 < chunks)
            def _():
                load(x, c + 2).start()

        @pl.when(me > 0)
        def _():
            send_y(c).wait_recv()

        @pl.when((me < last) & (c >= 4))
        def _():
            send_y(c - 4).wait_send()

    def after_forward(c):
        @pl.when(spill)
        def _():
            put_gu(c).start()

            @pl.when(c == 2)
            def _():
                get_gu(0).start()

    def forward(c, put):
        before_forward(c, put)

        @pl.when(me < last)
        def _():
            up_and_gate(c, True)

            @pl.when(me != 3)
            def _():
                send_y(c).start()

            @pl.when(me == 3)
            def _():
                relayed = among(c, BY_ON)

                @pl.when(~relayed)
                def _():
                    send_y(c).start()

                @pl.when(relayed)
                def _():
                    post_to(y_out, c, place(c, BY_ON), 0).start()

        @pl.when(me == last)
        def _():
            up_and_gate(c, False)

        after_forward(c)

    def hidden_back(c):
        slot = jnp.where(spill, 2 + (c & 1), c & 3)
        at, half = (c >> 1) & 1, c & 1
        by_y = dh[c]
        for j in range(ff // BACK):
            here = pl.ds(j * BACK, BACK)
            by_p = dot(wd[here, :], by_y).astype(BF).astype(F32)
            gate, up = gu[slot, here, :], gu[slot, pl.ds(ff + j * BACK, BACK), :]
            sig = jax.nn.sigmoid(gate)
            silu = gate * sig
            terms[at, 2, half, here, :] = (silu * up).astype(BF)
            terms[at, 1, half, here, :] = (silu * by_p).astype(BF)
            terms[at, 0, half, here, :] = (up * by_p * (sig + silu * (1 - sig))).astype(BF)

    def state_back(c):
        at, half = (c >> 1) & 1, c & 1
        wide = h[c].astype(F32)
        scale = scale_of(wide)
        by_a = (dot(wg[...], terms[at, 0, half]).astype(BF) + dot(wu[...], terms[at, 1, half]).astype(BF)).astype(F32)
        along = jnp.sum(by_a * wide, 0, keepdims=True) * (scale * scale * scale) * (1.0 / d)
        dh_out[c & 3] = dh[c] + (by_a * scale - wide * along).astype(BF)
        h[c] = (wide * scale).astype(BF)

    def before_backward(c, put):
        @pl.when(((c & 1) == 0) & ((c >> 1) >= later + 2))
        def _():
            keep_terms((c >> 1) - 2).wait()

        @pl.when(spill)
        def _():
            for k in (c, c + 1):
                @pl.when((put <= k) & (k < chunks))
                def _():
                    put_gu(k).wait()

            @pl.when(c + 1 < chunks)
            def _():
                get_gu(c + 1).start()

            get_gu(c).wait()

        @pl.when(me < last)
        def _():
            send_dh(c).wait_recv()

        @pl.when((me > 0) & (c >= 4))
        def _():
            send_dh(c - 4).wait_send()

    def after_backward(c):
        @pl.when(((c & 1) == 1) & ((c >> 1) >= later))
        def _():
            keep_terms(c >> 1).start()

            @pl.when(c == chunks - 1)
            def _():
                keep_terms(micro - 2).wait()
                fetch_terms(later).start()

    def backward(c, put):
        before_backward(c, put)

        @pl.when(me > 0)
        def _():
            hidden_back(c)
            state_back(c)

            @pl.when(me != 4)
            def _():
                send_dh(c).start()

            @pl.when(me == 4)
            def _():
                relayed = among(c, BY_OFF)

                @pl.when(~relayed)
                def _():
                    send_dh(c).start()

                @pl.when(relayed)
                def _():
                    post_to(dh_out, c, place(c, BY_OFF), 7).start()

        @pl.when(me == 0)
        def _():
            hidden_back(c)
            wide = h[c].astype(F32)
            h[c] = (wide * scale_of(wide)).astype(BF)

        after_backward(c)

    def add_terms(m, half):
        for j in range(ff // 2 // WIDTH):
            here = pl.ds(j * WIDTH, WIDTH)
            rows = pl.ds(pl.multiple_of(half * (ff // 2) + j * WIDTH, WIDTH), WIDTH)
            for lhs, i, total in ((h, 0, tg), (h, 1, tu), (dh, 2, td)):
                term = sum(dot(lhs[m * per + k], terms[m & 1, i, k, rows, :], NT) for k in range(per))
                total[half, :, here] += term.astype(BF).astype(F32)

    def weights_back(n):
        m, half = n >> 1, n & 1

        @pl.when((half == 0) & (m >= later))
        def _():
            @pl.when(m == later)
            def _():
                keep_terms(micro - 1).wait()
                fetch_terms(later + 1).start()

            fetch_terms(m).wait()

        add_terms(m, half)

        @pl.when((half == 1) & (m >= later) & (m + 2 < micro))
        def _():
            fetch_terms(m + 2).start()

    def hand_on(r):
        pltpu.make_async_remote_copy(
            src_ref=y_out.at[0], dst_ref=post.at[r], send_sem=y_send.at[0], recv_sem=post_recv.at[r],
            device_id={"pp": right}, device_id_type=MESH).wait_recv()

        @pl.when(me == 0)
        def _():
            post_on(r).start()

        @pl.when(me == last)
        def _():
            post_back(r).start()

    def word(q, carry):
        code = sum(jnp.where((me == s) & (q == i), number, 0) for s, row in enumerate(ORDER) for i, number in enumerate(row) if number)

        def operation(_, carry):
            code, on, back, done, handed, put = carry
            kind = code & 7

            @pl.when(kind == 1)
            def _():
                forward(on, put)

            @pl.when((kind == 1) & (me == 0) & (on == 2))
            def _():
                clear()

            @pl.when(kind == 2)
            def _():
                backward(back, put)

            @pl.when(kind == 3)
            def _():
                weights_back(done)

            @pl.when(kind == 4)
            def _():
                hand_on(handed)

            put = jnp.where(kind == 1, jnp.maximum(put, on - 1), put)
            put = jnp.where(kind == 2, jnp.maximum(put, jnp.minimum(back + 2, chunks)), put)
            one = [jnp.where(kind == k, 1, 0) for k in (1, 2, 3, 4)]
            return code >> 3, on + one[0], back + one[1], done + one[2], handed + one[3], put

        return lax.fori_loop(0, DIGITS, operation, (code, *carry))[1:]

    lax.fori_loop(0, max(len(row) for row in ORDER), word, (jnp.int32(0),) * 5)

    cut = ff // 2
    for i in (0, 1):
        wg[:, i * cut:(i + 1) * cut] = tg[i].astype(BF)
    out_g = pltpu.make_async_copy(wg, wg_out, w_sem.at[0])
    out_g.start()
    for i in (0, 1):
        wu[:, i * cut:(i + 1) * cut] = tu[i].astype(BF)
    out_u = pltpu.make_async_copy(wu, wu_out, w_sem.at[1])
    out_u.start()
    for i in (0, 1):
        wd[i * cut:(i + 1) * cut, :] = td[i].astype(BF).T
    out_d = pltpu.make_async_copy(wd, wd_out, w_sem.at[2])
    out_d.start()
    for copy in (out_g, out_u, out_d):
        copy.wait()

    @pl.when(me < last)
    def _():
        for c in range(chunks - 4, chunks):
            send_y(c).wait_send()

    @pl.when(me > 0)
    def _():
        for c in range(chunks - 4, chunks):
            send_dh(c).wait_send()

    def sent(r, _):
        post_on(r).wait_send()
        return 0

    lax.fori_loop(0, jnp.where(me == 0, len(BY_ON), jnp.where(me == last, len(BY_OFF), 0)), sent, 0)


def hand_out(*refs):
    for source, target in zip(refs[:3], refs[3:]):
        target[0] = source[...]


def solution(mesh):
    stages = mesh.shape["pp"]

    def step(x, dy, wg, wu, wd):
        micro, tokens, d = x.shape
        ff = wg.shape[2]
        per = tokens // T
        chunks = micro * per
        vmem, dma = pltpu.VMEM, pltpu.SemaphoreType.DMA
        hbm = pl.BlockSpec(memory_space=pl.ANY)
        outs = pl.pallas_call(
            functools.partial(kernel, stages),
            out_shape=(
                jax.ShapeDtypeStruct((d, ff), BF),
                jax.ShapeDtypeStruct((d, ff), BF),
                jax.ShapeDtypeStruct((ff, d), BF),
                jax.ShapeDtypeStruct((chunks, 2 * ff, T), F32),
                jax.ShapeDtypeStruct((16, d, T), BF),
                jax.ShapeDtypeStruct((micro, 3, per, ff, T), BF),
            ),
            in_specs=[hbm] * 5,
            out_specs=[hbm] * 6,
            scratch_shapes=[
                vmem((d, ff), BF), vmem((d, ff), BF), vmem((ff, d), BF),
                vmem((2, d, ff // 2), F32), vmem((2, d, ff // 2), F32), vmem((2, d, ff // 2), F32),
                vmem((chunks, d, T), BF), vmem((chunks, d, T), BF),
                vmem((4, 2 * ff, T), F32),
                vmem((RING, 3, per, ff, T), BF), vmem((ff, T), BF),
                vmem((4, d, T), BF), vmem((4, d, T), BF), vmem((2, T, d), BF),
                dma((3,)), dma((2,)), dma((2,)), dma((2,)), dma((4,)), dma((chunks,)), dma((4,)), dma((chunks,)), dma((16,)), dma((16,)), dma((2,)), dma((2,)),
            ],
            compiler_params=pltpu.CompilerParams(collective_id=0, has_side_effects=True, vmem_limit_bytes=67043328),
        )(x, dy, wg[0], wu[0], wd[0])
        cut = 2
        shapes = ((d, ff), (d, ff), (ff, d))
        return pl.pallas_call(
            hand_out,
            grid=(cut,),
            out_shape=tuple(jax.ShapeDtypeStruct((1, *shape), BF) for shape in shapes),
            in_specs=[pl.BlockSpec((r // cut, c), lambda i: (i, 0)) for r, c in shapes],
            out_specs=tuple(pl.BlockSpec((1, r // cut, c), lambda i: (0, i, 0)) for r, c in shapes),
        )(*outs[:3])

    return jax.shard_map(
        step,
        mesh=mesh,
        in_specs=(P("rep", None, None),) * 2 + (P("pp", None, None),) * 3,
        out_specs=(P(("rep", "pp"), None, None),) * 3,
        check_vma=False,
    )
```
